128 devices in a mesh: row: 32 (over y, x, core), col: 4 (over z).
Axes of the slice: x: 4, y: 4, z: 4, core: 2. Of those that a mesh axis runs over, the one named last changes fastest.
Arguments:
- stiff_bb: bfloat16 [384, 3, 128, 384], P(('row', 'col')), may hold values from -6 to 6
- stiff_bi: bfloat16 [384, 384, 3072], P(('row', 'col')), may hold values from -6 to 6
- constraint_modes: bfloat16 [384, 3072, 384], P(('row', 'col')), may hold values from -0.109375 to 0.109375
- interior_mass: float32 [384, 3072], P(('row', 'col')), may hold values from 0.25 to 4
- fixed_modes: bfloat16 [384, 3072, 256], P(('row', 'col')), may hold values from -6 to 6
- mass_bb: bfloat16 [384, 3, 128, 384], P(('row', 'col')), may hold values from -6 to 6
- boundary_map: int32 [384, 3], P(('row', 'col')), may hold values from 0 to 767, as said below
Outputs:
- interface_stiffness: float32 [768, 4, 128, 128], P('row', None, 'col')
- interface_mass: float32 [768, 4, 128, 128], P('row', None, 'col')
- mass_coupling: float32 [384, 256, 384], P(('row', 'col'))
The draws below stay inside these ranges and needn't reach their ends.
Inputs may be any that keep to these rules, and one draw needn't show every extreme that they name: `boundary_map`: row s holds blocks b, b + a, b + c with 0 < a < c < 4, all three in the range of one owner (block // 24). Rows come in aligned row groups of 12; no owner serves more than 1 row of one row group, and in every draw one owner serves exactly 1 row of every row group.
All inputs are finite; a program needn't handle non-finite values.
Results may differ from the reference program's by a relative error of at most 0.0029.
Values sent between devices are 32-bit elements; how exact they have to be, the bound alone decides.
No kernel may reach another device: no remote copies, remote signals or barrier semaphores. Data moves between devices by JAX's collectives and lax.ppermute only.
A program may use at most 192 MiB of HBM per device.

```python
import math
import jax
import jax.numpy as jnp
from jax import lax

NI = 3072
BLK = 128
NB = 384
NM = 256
BAND = 4
BPO = 24
SE_GRP = 12
CAP = 1
SETOT = 384
NBLOCK = 768
N_ROW = 32


def draw_boundary_map(key, part):
    slot_count = N_ROW * CAP
    keys = jax.random.split(jax.random.fold_in(key, 17), 7)
    priority_tiers = jax.random.randint(keys[0], (N_ROW,), 0, 4)
    busiest_targets = jax.random.randint(keys[1], (), 0, N_ROW)
    position_owner = jnp.arange(slot_count) // CAP
    random_jitter = jax.random.randint(keys[2], (N_ROW, slot_count), 0, 65536)
    extra_credit = jnp.where(position_owner == busiest_targets, 1 << 20, 0)
    ranking_values = random_jitter + priority_tiers[position_owner][None, :] * 16384 + extra_credit[None, :]
    ranking_values = ranking_values * slot_count + jnp.arange(slot_count)[None, :]
    picked = lax.top_k(ranking_values, SE_GRP)[1]
    order_scores = jax.random.randint(keys[3], (N_ROW, SE_GRP), 0, 4096) * SE_GRP + jnp.arange(SE_GRP)[None, :]
    order = lax.top_k(order_scores, SE_GRP)[1]
    picked = jnp.take_along_axis(picked, order, axis=1)
    owners = (picked // CAP).reshape(SETOT)
    first = jax.random.randint(keys[4], (SETOT,), 1, BAND - 1)
    second = first + jax.random.randint(keys[5], (SETOT,), 1, BAND - first)
    start = owners * BPO + jax.random.randint(keys[6], (SETOT,), 0, BPO - second)
    return jnp.stack([start, start + first, start + second], axis=1).astype(jnp.int32)


def steps_of(rng, extent, cuts, low, top_value):
    gain, own = 1.0, jax.random.fold_in(rng, 6)
    for position, blocks in cuts:
        steps = jnp.exp(jax.random.uniform(jax.random.fold_in(own, position), (blocks,), jnp.float32, low / len(cuts), top_value / len(cuts)))
        gain = gain * jnp.repeat(steps, extent[position] // blocks).reshape([-1 if axis == position else 1 for axis in range(len(extent))])
    return gain


def centred(key, extent, deviation, most, pieces=(), dtype=jnp.bfloat16):
    array = deviation * jax.random.normal(key, extent, jnp.float32)
    if pieces:
        array = array * steps_of(key, extent, pieces, -0.22, 0.18)
    return jnp.clip(array, -most, most).astype(dtype)


def setup_inputs(seed: int = 0) -> dict:
    streams_of = jax.random.split(jax.random.key(seed), 8)
    return {
        "stiff_bb": centred(streams_of[0], (SETOT, 3, BLK, NB), 1.0, 6.0, ((0, 128),)),
        "stiff_bi": centred(streams_of[1], (SETOT, NB, NI), 1.0, 6.0, ((0, 128),)),
        "constraint_modes": centred(streams_of[2], (SETOT, NI, NB), NI ** -0.5, 0.109375, ((0, 128),)),
        "interior_mass": jnp.clip(jnp.exp(math.log(4.0) - 2.7725887 * jax.random.uniform(streams_of[3], (SETOT, NI), jnp.float32) ** steps_of(streams_of[3], (SETOT, NI), ((0, 128),), -0.2, 0.2)), 0.25, 4.0),
        "fixed_modes": centred(streams_of[4], (SETOT, NI, NM), 1.0, 6.0, ((0, 128),)),
        "mass_bb": centred(streams_of[5], (SETOT, 3, BLK, NB), 1.0, 6.0, ((0, 128),)),
        "boundary_map": draw_boundary_map(jax.random.fold_in(streams_of[7], 71), 0),
    }


PAIRS = ((0, 0), (1, 1), (2, 2), (0, 1), (0, 2), (1, 2))


def reduce_one(items):
    block_bb, block_bi, psi, masses, modes, mass_block = items
    order = block_bi.shape[0]
    weighted = (masses[:, None] * psi.astype(jnp.float32)).astype(jnp.bfloat16)
    red_k = block_bb.reshape(order, order).astype(jnp.float32) + jnp.dot(block_bi, psi, preferred_element_type=jnp.float32)
    red_m = mass_block.reshape(order, order).astype(jnp.float32) + jnp.dot(psi.T, weighted, preferred_element_type=jnp.float32)
    coupling = jnp.dot(modes.T, weighted, preferred_element_type=jnp.float32)
    return red_k, red_m, coupling


def reference(stiff_bb, stiff_bi, constraint_modes, interior_mass, fixed_modes, mass_bb, boundary_map):
    red_k, red_m, coupling = lax.map(reduce_one, (stiff_bb, stiff_bi, constraint_modes, interior_mass, fixed_modes, mass_bb))
    width = stiff_bb.shape[2]
    total_k = jnp.zeros((NBLOCK, BAND, width, width), jnp.float32)
    total_m = jnp.zeros((NBLOCK, BAND, width, width), jnp.float32)
    for first, second in PAIRS:
        rows = boundary_map[:, first].astype(jnp.int32)
        offset = (boundary_map[:, second] - boundary_map[:, first]).astype(jnp.int32)
        piece_k = red_k[:, first * width:(first + 1) * width, second * width:(second + 1) * width]
        piece_m = red_m[:, first * width:(first + 1) * width, second * width:(second + 1) * width]
        total_k = total_k.at[rows, offset].add(piece_k)
        total_m = total_m.at[rows, offset].add(piece_m)
    return total_k, total_m, coupling
```

```python
import functools

import jax
import jax.numpy as jnp
from jax import lax
from jax.experimental import pallas as pl
from jax.experimental.pallas import tpu as pltpu
from jax.sharding import PartitionSpec as P

BAND = 4
BPO = 24
PAIRS = ((0, 0), (1, 1), (2, 2), (0, 1), (0, 2), (1, 2))
ROWS = 32
HEAD = 6 * ROWS
PKT = HEAD + 8
STEP = 1024


F32 = jnp.float32
VMEM = pl.BlockSpec(memory_space=pltpu.VMEM)
SMEM = pl.BlockSpec(memory_space=pltpu.SMEM)


def pkt(count):
    return jax.ShapeDtypeStruct((count, PKT, 128), F32)


def write_packets(s, total, map_ref, outs):
    first = map_ref[s, 0]
    owner = first // BPO
    code = owner * BPO + (first - owner * BPO)
    code = (code * 4 + map_ref[s, 1] - first) * 4 + map_ref[s, 2] - first
    head = jnp.full((8, 128), code.astype(F32), F32)
    me = lax.axis_index("col")
    for d, out in enumerate(outs):
        lane = lax.rem(me + d, 4)
        for p, (i, j) in enumerate(PAIRS):
            rows = pl.ds(pl.multiple_of(i * 128 + lane * ROWS, ROWS), ROWS)
            out[0, p * ROWS : (p + 1) * ROWS, :] = total[rows, j * 128 : (j + 1) * 128]
        out[0, HEAD:PKT, :] = head


def k_kernel(steps, map_ref, bb, bi, cm, o0, o1, o2, o3, total):
    s, k = pl.program_id(0), pl.program_id(1)

    @pl.when(k == 0)
    def _():
        for i in range(3):
            total[i * 128 : (i + 1) * 128, :] = bb[0, i].astype(F32)

    total[0:128, :] += jnp.dot(bi[0, 0:128, :], cm[0], preferred_element_type=F32)
    total[128:384, 128:384] += jnp.dot(
        bi[0, 128:384, :], cm[0, :, 128:384], preferred_element_type=F32
    )

    @pl.when(k == steps - 1)
    def _():
        write_packets(s, total, map_ref, (o0, o1, o2, o3))


def k_packets(bmap, stiff_bb, stiff_bi, cm):
    count, order, inner = stiff_bi.shape
    steps = inner // STEP
    return pl.pallas_call(
        functools.partial(k_kernel, steps),
        grid=(count, steps),
        in_specs=[
            SMEM,
            pl.BlockSpec((1, 3, 128, order), lambda s, k: (s, 0, 0, 0)),
            pl.BlockSpec((1, order, STEP), lambda s, k: (s, 0, k)),
            pl.BlockSpec((1, STEP, order), lambda s, k: (s, k, 0)),
        ],
        out_specs=[pl.BlockSpec((1, PKT, 128), lambda s, k: (s, 0, 0))] * 4,
        out_shape=[pkt(count)] * 4,
        scratch_shapes=[pltpu.VMEM((order, order), F32)],
        cost_estimate=pl.CostEstimate(
            flops=6 * count * 128 * 128 * inner * 2, bytes_accessed=16000000, transcendentals=0
        ),
        name="stiffness",
    )(bmap, stiff_bb, stiff_bi, cm)


def m_kernel(steps, map_ref, bb, im, cm, fm, o0, o1, o2, o3, coup, total, w):
    s, k = pl.program_id(0), pl.program_id(1)

    @pl.when(k == 0)
    def _():
        for i in range(3):
            total[i * 128 : (i + 1) * 128, :] = bb[0, i].astype(F32)
        coup[...] = jnp.zeros_like(coup)

    for j in range(STEP // 128):
        lines = im[:, pl.ds(pl.multiple_of(k * STEP + j * 128, 128), 128)]
        mine = lax.broadcasted_iota(jnp.int32, lines.shape, 0) == s
        line = jnp.sum(jnp.where(mine, lines, 0.0), axis=0, keepdims=True)
        column = jnp.broadcast_to(line, (128, 128)).T
        part = slice(j * 128, (j + 1) * 128)
        for i in range(3):
            lanes = slice(i * 128, (i + 1) * 128)
            w[part, lanes] = (column * cm[0, part, lanes].astype(F32)).astype(jnp.bfloat16)
    dims = (((0,), (0,)), ((), ()))
    total[0:128, :] += lax.dot_general(cm[0, :, 0:128], w[...], dims, preferred_element_type=F32)
    total[128:384, 128:384] += lax.dot_general(
        cm[0, :, 128:384], w[:, 128:384], dims, preferred_element_type=F32
    )
    coup[0] += lax.dot_general(fm[0], w[...], dims, preferred_element_type=F32)

    @pl.when(k == steps - 1)
    def _():
        write_packets(s, total, map_ref, (o0, o1, o2, o3))


def m_packets(bmap, mass_bb, im, cm, fm):
    count, inner, order = cm.shape
    modes = fm.shape[2]
    steps = inner // STEP
    return pl.pallas_call(
        functools.partial(m_kernel, steps),
        grid=(count, steps),
        in_specs=[
            SMEM,
            pl.BlockSpec((1, 3, 128, order), lambda s, k: (s, 0, 0, 0)),
            pl.BlockSpec((count, inner), lambda s, k: (0, 0)),
            pl.BlockSpec((1, STEP, order), lambda s, k: (s, k, 0)),
            pl.BlockSpec((1, STEP, modes), lambda s, k: (s, k, 0)),
        ],
        out_specs=[pl.BlockSpec((1, PKT, 128), lambda s, k: (s, 0, 0))] * 4
        + [pl.BlockSpec((1, modes, order), lambda s, k: (s, 0, 0))],
        out_shape=[pkt(count)] * 4 + [jax.ShapeDtypeStruct((count, modes, order), F32)],
        scratch_shapes=[pltpu.VMEM((order, order), F32), pltpu.VMEM((STEP, order), jnp.bfloat16)],
        cost_estimate=pl.CostEstimate(
            flops=12 * count * 128 * 128 * inner * 2, bytes_accessed=14000000, transcendentals=0
        ),
        name="mass",
    )(bmap, mass_bb, im, cm, fm)


def code_of(ref, n):
    return jnp.max(ref[n, HEAD : HEAD + 1, :]).astype(jnp.int32)


def place():
    r = lax.axis_index("row")
    core = lax.rem(r, 2)
    x = lax.rem(r // 2, 4)
    y = r // 8
    u = jnp.where(core == 0, x, y)
    v = jnp.where(core == 0, y, x)
    return core, u, v


def pack_kernel(i0, i1, i2, i3, o0, o1, o2, o3):
    core, u, v = place()
    outs = (o0, o1, o2, o3)
    empty = jnp.full((8, 128), -1.0, F32)
    for out in outs:
        for n in range(8):
            out[n, HEAD:PKT, :] = empty
    for ref in (i0, i1, i2, i3):
        for n in range(ref.shape[0]):
            owner = code_of(ref, n) // (BPO * 16)
            c = lax.rem(owner, 2)
            x = lax.rem(owner // 2, 4)
            y = owner // 8
            du = lax.rem(jnp.where(core == 0, x, y) - u + 4, 4)
            dv = lax.rem(jnp.where(core == 0, y, x) - v + 4, 4)
            slot = dv * 2 + lax.rem(c + core, 2)
            for k, out in enumerate(outs):

                @pl.when(du == k)
                def _(out=out, ref=ref, n=n):
                    out[slot] = ref[n]


def pack(bufs):
    return pl.pallas_call(
        pack_kernel,
        in_specs=[VMEM] * 4,
        out_specs=[VMEM] * 4,
        out_shape=[pkt(8)] * 4,
        cost_estimate=pl.CostEstimate(flops=2000000, bytes_accessed=4000000, transcendentals=0),
        name="pack",
    )(*bufs)


def turn_kernel(*refs):
    for src in range(4):
        for q in range(8):
            refs[4 + q][src] = refs[src][q]


def turn(bufs):
    return pl.pallas_call(
        turn_kernel,
        in_specs=[VMEM] * 4,
        out_specs=[VMEM] * 8,
        out_shape=[pkt(4)] * 8,
        cost_estimate=pl.CostEstimate(flops=2000000, bytes_accessed=6000000, transcendentals=0),
        name="turn",
    )(*bufs)


def sum_kernel(*refs):
    band = refs[-1]
    band[...] = jnp.zeros_like(band)
    for ref in refs[:-1]:
        for n in range(ref.shape[0]):
            code = code_of(ref, n)

            @pl.when(code >= 0)
            def _(ref=ref, n=n, code=code):
                last = lax.rem(code, 4)
                mid = lax.rem(code // 4, 4)
                base = lax.rem(code // 16, BPO)
                marks = (0, mid, last)
                for p, (i, j) in enumerate(PAIRS):
                    g = base + marks[i]
                    d = marks[j] - marks[i]
                    band[g, d] += ref[n, p * ROWS : (p + 1) * ROWS, :]


def assemble(bufs):
    return pl.pallas_call(
        sum_kernel,
        in_specs=[VMEM] * len(bufs),
        out_specs=VMEM,
        out_shape=jax.ShapeDtypeStruct((BPO, BAND, ROWS, 128), F32),
        cost_estimate=pl.CostEstimate(flops=4000000, bytes_accessed=6000000, transcendentals=0),
        name="assemble",
    )(*bufs)


def spots():
    return [(r // 8, (r // 2) % 4, r % 2) for r in range(32)]


def row_of(y, x, c):
    return (y % 4) * 8 + (x % 4) * 2 + c


def first_turn(d):
    return [
        (r, row_of(y, x + d, c) if c == 0 else row_of(y + d, x, c))
        for r, (y, x, c) in enumerate(spots())
    ]


def second_turn(d, e):
    return [
        (r, row_of(y + d, x, c ^ e) if c == 0 else row_of(y, x + d, c ^ e))
        for r, (y, x, c) in enumerate(spots())
    ]


def over_col(bufs):
    return [bufs[0]] + [
        lax.ppermute(bufs[d], "col", [(z, (z + d) % 4) for z in range(4)]) for d in (1, 2, 3)
    ]


def over_row(bufs):
    slots = pack(bufs)
    slots = [slots[0]] + [lax.ppermute(slots[d], "row", first_turn(d)) for d in (1, 2, 3)]
    parts = turn(slots)
    return [parts[0]] + [
        lax.ppermute(parts[q], "row", second_turn(q // 2, q % 2)) for q in (2, 3, 4, 5, 6, 7, 1)
    ]


def per_device(
    stiff_bb, stiff_bi, constraint_modes, interior_mass, fixed_modes, mass_bb, boundary_map
):
    k_out = k_packets(boundary_map, stiff_bb, stiff_bi, constraint_modes)
    k_in = over_col(k_out)
    *m_out, coupling = m_packets(
        boundary_map, mass_bb, interior_mass, constraint_modes, fixed_modes
    )
    m_in = over_col(m_out)
    band_k = assemble(over_row(k_in))
    band_m = assemble(over_row(m_in))
    return band_k, band_m, coupling


def solution(mesh):
    placed = (
        P(("row", "col"), None, None, None),
        P(("row", "col"), None, None),
        P(("row", "col"), None, None),
        P(("row", "col"), None),
        P(("row", "col"), None, None),
        P(("row", "col"), None, None, None),
        P(("row", "col"), None),
    )
    return jax.shard_map(
        per_device,
        mesh=mesh,
        in_specs=placed,
        out_specs=(
            P("row", None, "col", None),
            P("row", None, "col", None),
            P(("row", "col"), None, None),
        ),
        check_vma=False,
    )
```

```python
import functools

import jax
import jax.numpy as jnp
from jax import lax
from jax.experimental import pallas as pl
from jax.experimental.pallas import tpu as pltpu
from jax.sharding import PartitionSpec as P

BAND = 4
BPO = 24
PAIRS = ((0, 0), (1, 1), (2, 2), (0, 1), (0, 2), (1, 2))
ROWS = 32
HEAD = 6 * ROWS
PKT = HEAD + 8
STEP = 1024


F32 = jnp.float32
VMEM = pl.BlockSpec(memory_space=pltpu.VMEM)
SMEM = pl.BlockSpec(memory_space=pltpu.SMEM)
ANY = pl.BlockSpec(memory_space=pl.ANY)


def pkt(count):
    return jax.ShapeDtypeStruct((count, PKT, 128), F32)


def write_packets(s, total, map_ref, outs):
    first = map_ref[s, 0]
    owner = first // BPO
    code = owner * BPO + (first - owner * BPO)
    code = (code * 4 + map_ref[s, 1] - first) * 4 + map_ref[s, 2] - first
    head = jnp.full((8, 128), code.astype(F32), F32)
    me = lax.axis_index("col")
    for d, out in enumerate(outs):
        lane = lax.rem(me + d, 4)
        for p, (i, j) in enumerate(PAIRS):
            rows = pl.ds(pl.multiple_of(i * 128 + lane * ROWS, ROWS), ROWS)
            out[0, p * ROWS : (p + 1) * ROWS, :] = total[rows, j * 128 : (j + 1) * 128]
        out[0, HEAD:PKT, :] = head


def k_kernel(map_ref, bb, bi, cm, o0, o1, o2, o3, total):
    for i in range(3):
        total[i * 128 : (i + 1) * 128, :] = bb[0, i].astype(F32)
    total[0:128, :] += jnp.dot(bi[0, 0:128, :], cm[0], preferred_element_type=F32)
    total[128:384, 128:384] += jnp.dot(
        bi[0, 128:384, :], cm[0, :, 128:384], preferred_element_type=F32
    )
    write_packets(pl.program_id(0), total, map_ref, (o0, o1, o2, o3))


def k_packets(bmap, stiff_bb, stiff_bi, cm):
    count, order, inner = stiff_bi.shape
    return pl.pallas_call(
        k_kernel,
        grid=(count,),
        in_specs=[
            SMEM,
            pl.BlockSpec((1, 3, 128, order), lambda s: (s, 0, 0, 0)),
            pl.BlockSpec((1, order, inner), lambda s: (s, 0, 0)),
            pl.BlockSpec((1, inner, order), lambda s: (s, 0, 0)),
        ],
        out_specs=[pl.BlockSpec((1, PKT, 128), lambda s: (s, 0, 0))] * 4,
        out_shape=[pkt(count)] * 4,
        scratch_shapes=[pltpu.VMEM((order, order), F32)],
        compiler_params=pltpu.CompilerParams(vmem_limit_bytes=24 << 20),
        cost_estimate=pl.CostEstimate(
            flops=6 * count * 128 * 128 * inner * 2, bytes_accessed=16000000, transcendentals=0
        ),
        name="stiffness",
    )(bmap, stiff_bb, stiff_bi, cm)


def m_kernel(steps, map_ref, bb, im, cm, fm, after, o0, o1, o2, o3, coup, total, w):
    s, k = pl.program_id(0), pl.program_id(1)

    @pl.when(k == 0)
    def _():
        for i in range(3):
            total[i * 128 : (i + 1) * 128, :] = bb[0, i].astype(F32)
        coup[...] = jnp.zeros_like(coup)

    for j in range(STEP // 128):
        lines = im[:, pl.ds(pl.multiple_of(k * STEP + j * 128, 128), 128)]
        mine = lax.broadcasted_iota(jnp.int32, lines.shape, 0) == s
        line = jnp.sum(jnp.where(mine, lines, 0.0), axis=0, keepdims=True)
        column = jnp.broadcast_to(line, (128, 128)).T
        part = slice(j * 128, (j + 1) * 128)
        for i in range(3):
            lanes = slice(i * 128, (i + 1) * 128)
            w[part, lanes] = (column * cm[0, part, lanes].astype(F32)).astype(jnp.bfloat16)
    dims = (((0,), (0,)), ((), ()))
    total[0:128, :] += lax.dot_general(cm[0, :, 0:128], w[...], dims, preferred_element_type=F32)
    total[128:384, 128:384] += lax.dot_general(
        cm[0, :, 128:384], w[:, 128:384], dims, preferred_element_type=F32
    )
    coup[0] += lax.dot_general(fm[0], w[...], dims, preferred_element_type=F32)

    @pl.when(k == steps - 1)
    def _():
        write_packets(s, total, map_ref, (o0, o1, o2, o3))


def m_packets(bmap, mass_bb, im, cm, fm, after):
    count, inner, order = cm.shape
    modes = fm.shape[2]
    steps = inner // STEP
    return pl.pallas_call(
        functools.partial(m_kernel, steps),
        grid=(count, steps),
        in_specs=[
            SMEM,
            pl.BlockSpec((1, 3, 128, order), lambda s, k: (s, 0, 0, 0)),
            pl.BlockSpec((count, inner), lambda s, k: (0, 0)),
            pl.BlockSpec((1, STEP, order), lambda s, k: (s, k, 0)),
            pl.BlockSpec((1, STEP, modes), lambda s, k: (s, k, 0)),
            ANY,
        ],
        compiler_params=pltpu.CompilerParams(vmem_limit_bytes=24 << 20),
        out_specs=[pl.BlockSpec((1, PKT, 128), lambda s, k: (s, 0, 0))] * 4
        + [pl.BlockSpec((1, modes, order), lambda s, k: (s, 0, 0))],
        out_shape=[pkt(count)] * 4 + [jax.ShapeDtypeStruct((count, modes, order), F32)],
        scratch_shapes=[pltpu.VMEM((order, order), F32), pltpu.VMEM((STEP, order), jnp.bfloat16)],
        cost_estimate=pl.CostEstimate(
            flops=12 * count * 128 * 128 * inner * 2, bytes_accessed=14000000, transcendentals=0
        ),
        name="mass",
    )(bmap, mass_bb, im, cm, fm, after)


SMALL = pltpu.CompilerParams(vmem_limit_bytes=12 << 20)


def codes_of(heads, count):
    return [jnp.max(heads[n, 0:1, :]).astype(jnp.int32) for n in range(count)]


def run(copies):
    for copy in copies:
        copy.start()
    for copy in copies:
        copy.wait()


def place():
    r = lax.axis_index("row")
    core = lax.rem(r, 2)
    x = lax.rem(r // 2, 4)
    y = r // 8
    u = jnp.where(core == 0, x, y)
    v = jnp.where(core == 0, y, x)
    return core, u, v


def pack_kernel(i0, i1, i2, i3, o0, o1, o2, o3, held, empty, sems):
    core, u, v = place()
    outs = (o0, o1, o2, o3)
    count = i0.shape[0]
    empty[...] = jnp.full(empty.shape, -1.0, F32)
    loads = [
        pltpu.make_async_copy(ref, held.at[pl.ds(k * count, count)], sems.at[k])
        for k, ref in enumerate((i0, i1, i2, i3))
    ]
    clears = [
        pltpu.make_async_copy(empty, out.at[:, pl.ds(HEAD, 8), :], sems.at[4 + k])
        for k, out in enumerate(outs)
    ]
    run(loads + clears)
    owners = [
        jnp.max(held[n, HEAD : HEAD + 1, :]).astype(jnp.int32) // (BPO * 16)
        for n in range(4 * count)
    ]
    for n, owner in enumerate(owners):
        c = lax.rem(owner, 2)
        x = lax.rem(owner // 2, 4)
        y = owner // 8
        du = lax.rem(jnp.where(core == 0, x, y) - u + 4, 4)
        dv = lax.rem(jnp.where(core == 0, y, x) - v + 4, 4)
        slot = dv * 2 + lax.rem(c + core, 2)
        for k, out in enumerate(outs):

            @pl.when(du == k)
            def _(out=out, n=n, slot=slot):
                pltpu.make_async_copy(held.at[n], out.at[slot], sems.at[8 + n]).start()

    for n in range(4 * count):
        pltpu.make_async_copy(held.at[n], o0.at[0], sems.at[8 + n]).wait()


def pack(bufs):
    count = bufs[0].shape[0]
    return pl.pallas_call(
        pack_kernel,
        in_specs=[ANY] * 4,
        out_specs=[ANY] * 4,
        out_shape=[pkt(8)] * 4,
        scratch_shapes=[
            pltpu.VMEM((4 * count, PKT, 128), F32),
            pltpu.VMEM((8, 8, 128), F32),
            pltpu.SemaphoreType.DMA((8 + 4 * count,)),
        ],
        compiler_params=SMALL,
        cost_estimate=pl.CostEstimate(flops=2000000, bytes_accessed=4000000, transcendentals=0),
        name="pack",
    )(*bufs)


def turn_kernel(*refs):
    ins, outs, held, sems = refs[:4], refs[4:11], refs[11], refs[12]
    loads = [pltpu.make_async_copy(ref, held.at[k], sems.at[k]) for k, ref in enumerate(ins)]
    stores = []
    for copy in loads:
        copy.start()
    for k in range(4):
        loads[k].wait()
        for q in range(1, 8):
            copy = pltpu.make_async_copy(
                held.at[k, q], outs[q - 1].at[k], sems.at[4 + 7 * k + q - 1]
            )
            copy.start()
            stores.append(copy)
    for copy in stores:
        copy.wait()


def turn(bufs):
    return pl.pallas_call(
        turn_kernel,
        in_specs=[ANY] * 4,
        out_specs=[ANY] * 7,
        out_shape=[pkt(4)] * 7,
        scratch_shapes=[
            pltpu.VMEM((4, 8, PKT, 128), F32),
            pltpu.SemaphoreType.DMA((32,)),
        ],
        compiler_params=SMALL,
        cost_estimate=pl.CostEstimate(flops=2000000, bytes_accessed=6000000, transcendentals=0),
        name="turn",
    )(*bufs)


def sum_kernel(*refs):
    ins, band, heads, held, sems = refs[:11], refs[11], refs[12], refs[13], refs[14]
    slots = [(ref, 0) for ref in ins[:4]] + [(ref, n) for ref in ins[4:] for n in range(4)]
    loads = []
    for k in range(4):
        loads.append(
            pltpu.make_async_copy(ins[k].at[0, pl.ds(HEAD, 8), :], heads.at[k], sems.at[k])
        )
    for k in range(7):
        loads.append(
            pltpu.make_async_copy(
                ins[4 + k].at[:, pl.ds(HEAD, 8), :], heads.at[pl.ds(4 + 4 * k, 4)], sems.at[4 + k]
            )
        )
    run(loads)
    codes = codes_of(heads, len(slots))

    def fetch(n):
        ref, k = slots[n]
        return pltpu.make_async_copy(ref.at[k, pl.ds(0, HEAD), :], held.at[n], sems.at[n])

    for n, code in enumerate(codes):

        @pl.when(code >= 0)
        def _(n=n):
            fetch(n).start()

    band[...] = jnp.zeros_like(band)
    for n, code in enumerate(codes):

        @pl.when(code >= 0)
        def _(n=n, code=code):
            last = lax.rem(code, 4)
            mid = lax.rem(code // 4, 4)
            base = lax.rem(code // 16, BPO)
            marks = (0, mid, last)
            fetch(n).wait()
            for p, (i, j) in enumerate(PAIRS):
                g = base + marks[i]
                d = marks[j] - marks[i]
                band[g, d] += held[n, p * ROWS : (p + 1) * ROWS, :]


def assemble(bufs):
    return pl.pallas_call(
        sum_kernel,
        in_specs=[ANY] * len(bufs),
        out_specs=VMEM,
        out_shape=jax.ShapeDtypeStruct((BPO, BAND, ROWS, 128), F32),
        scratch_shapes=[
            pltpu.VMEM((32, 8, 128), F32),
            pltpu.VMEM((32, HEAD, 128), F32),
            pltpu.SemaphoreType.DMA((32,)),
        ],
        compiler_params=SMALL,
        cost_estimate=pl.CostEstimate(flops=4000000, bytes_accessed=6000000, transcendentals=0),
        name="assemble",
    )(*bufs)


def spots():
    return [(r // 8, (r // 2) % 4, r % 2) for r in range(32)]


def row_of(y, x, c):
    return (y % 4) * 8 + (x % 4) * 2 + c


def first_turn(d):
    return [
        (r, row_of(y, x + d, c) if c == 0 else row_of(y + d, x, c))
        for r, (y, x, c) in enumerate(spots())
    ]


def second_turn(d, e):
    return [
        (r, row_of(y + d, x, c ^ e) if c == 0 else row_of(y, x + d, c ^ e))
        for r, (y, x, c) in enumerate(spots())
    ]


def over_col(bufs):
    return [bufs[0]] + [
        lax.ppermute(bufs[d], "col", [(z, (z + d) % 4) for z in range(4)]) for d in (1, 2, 3)
    ]


def over_row(bufs):
    slots = pack(bufs)
    slots = [slots[0]] + [lax.ppermute(slots[d], "row", first_turn(d)) for d in (1, 2, 3)]
    parts = turn(slots)
    return slots + [
        lax.ppermute(parts[q - 1], "row", second_turn(q // 2, q % 2))
        for q in (2, 3, 4, 5, 6, 7, 1)
    ]


def per_device(
    stiff_bb, stiff_bi, constraint_modes, interior_mass, fixed_modes, mass_bb, boundary_map
):
    k_out = k_packets(boundary_map, stiff_bb, stiff_bi, constraint_modes)
    k_in = over_col(k_out)
    *m_out, coupling = m_packets(
        boundary_map, mass_bb, interior_mass, constraint_modes, fixed_modes, k_out[0]
    )
    m_in = over_col(m_out)
    band_k = assemble(over_row(k_in))
    band_m = assemble(over_row(m_in))
    return band_k, band_m, coupling


def solution(mesh):
    placed = (
        P(("row", "col"), None, None, None),
        P(("row", "col"), None, None),
        P(("row", "col"), None, None),
        P(("row", "col"), None),
        P(("row", "col"), None, None),
        P(("row", "col"), None, None, None),
        P(("row", "col"), None),
    )
    return jax.shard_map(
        per_device,
        mesh=mesh,
        in_specs=placed,
        out_specs=(
            P("row", None, "col", None),
            P("row", None, "col", None),
            P(("row", "col"), None, None),
        ),
        check_vma=False,
    )
```

```python
import functools

import jax
import jax.numpy as jnp
from jax import lax
from jax.experimental import pallas as pl
from jax.experimental.pallas import tpu as pltpu
from jax.sharding import PartitionSpec as P


BAND = 4
BPO = 24
PAIRS = ((0, 0), (1, 1), (2, 2), (0, 1), (0, 2), (1, 2))
ROWS = 32
HEAD = 6 * ROWS
PKT = HEAD + 8
STEP = 1024


F32 = jnp.float32
VMEM = pl.BlockSpec(memory_space=pltpu.VMEM)
SMEM = pl.BlockSpec(memory_space=pltpu.SMEM)
ANY = pl.BlockSpec(memory_space=pl.ANY)
HBM = pl.BlockSpec(memory_space=pltpu.HBM)


def write_packets(s, total, map_ref, outs):
    me = lax.axis_index("col")
    for d, out in enumerate(outs):
        lane = lax.rem(me + d, 4)
        for p, (i, j) in enumerate(PAIRS):
            rows = pl.ds(pl.multiple_of(i * 128 + lane * ROWS, ROWS), ROWS)
            out[s, p * ROWS : (p + 1) * ROWS, :] = total[rows, j * 128 : (j + 1) * 128]
    if map_ref is not None:
        first = map_ref[s, 0]
        code = (first * 4 + map_ref[s, 1] - first) * 4 + map_ref[s, 2] - first
        head = jnp.full((8, 128), code.astype(F32), F32)
        for out in outs:
            out[s, HEAD:PKT, :] = head


def k_kernel(map_ref, bb, bi, cm, o0, o1, o2, o3, total):
    for i in range(3):
        total[i * 128 : (i + 1) * 128, :] = bb[0, i].astype(F32)
    total[0:128, :] += jnp.dot(bi[0, 0:128, :], cm[0], preferred_element_type=F32)
    total[128:384, 128:384] += jnp.dot(
        bi[0, 128:384, :], cm[0, :, 128:384], preferred_element_type=F32
    )
    write_packets(pl.program_id(0), total, map_ref, (o0, o1, o2, o3))


def k_packets(bmap, stiff_bb, stiff_bi, cm):
    count, order, inner = stiff_bi.shape
    return pl.pallas_call(
        k_kernel,
        grid=(count,),
        in_specs=[
            SMEM,
            pl.BlockSpec((1, 3, 128, order), lambda s: (s, 0, 0, 0)),
            pl.BlockSpec((1, order, inner), lambda s: (s, 0, 0)),
            pl.BlockSpec((1, inner, order), lambda s: (s, 0, 0)),
        ],
        out_specs=[VMEM] * 4,
        out_shape=[held(count, PKT)] * 4,
        scratch_shapes=[pltpu.VMEM((order, order), F32)],
        compiler_params=pltpu.CompilerParams(vmem_limit_bytes=56 << 20),
        cost_estimate=pl.CostEstimate(
            flops=6 * count * 128 * 128 * inner * 2, bytes_accessed=16000000, transcendentals=0
        ),
        name="stiffness",
    )(bmap, stiff_bb, stiff_bi, cm)


def m_kernel(steps, bb, im, cm, fm, o0, o1, o2, o3, coup, total, w):
    s, k = pl.program_id(0), pl.program_id(1)

    @pl.when(k == 0)
    def _():
        for i in range(3):
            total[i * 128 : (i + 1) * 128, :] = bb[0, i].astype(F32)
        coup[...] = jnp.zeros_like(coup)

    for j in range(STEP // 128):
        lines = im[:, pl.ds(pl.multiple_of(k * STEP + j * 128, 128), 128)]
        mine = lax.broadcasted_iota(jnp.int32, lines.shape, 0) == s
        line = jnp.sum(jnp.where(mine, lines, 0.0), axis=0, keepdims=True)
        column = jnp.broadcast_to(line, (128, 128)).T
        part = slice(j * 128, (j + 1) * 128)
        for i in range(3):
            lanes = slice(i * 128, (i + 1) * 128)
            w[part, lanes] = (column * cm[0, part, lanes].astype(F32)).astype(jnp.bfloat16)
    dims = (((0,), (0,)), ((), ()))
    total[0:128, :] += lax.dot_general(cm[0, :, 0:128], w[...], dims, preferred_element_type=F32)
    total[128:384, 128:384] += lax.dot_general(
        cm[0, :, 128:384], w[:, 128:384], dims, preferred_element_type=F32
    )
    coup[0] += lax.dot_general(fm[0], w[...], dims, preferred_element_type=F32)

    @pl.when(k == steps - 1)
    def _():
        write_packets(s, total, None, (o0, o1, o2, o3))


def m_packets(mass_bb, im, cm, fm):
    count, inner, order = cm.shape
    modes = fm.shape[2]
    steps = inner // STEP
    return pl.pallas_call(
        functools.partial(m_kernel, steps),
        grid=(count, steps),
        in_specs=[
            pl.BlockSpec((1, 3, 128, order), lambda s, k: (s, 0, 0, 0)),
            pl.BlockSpec((count, inner), lambda s, k: (0, 0)),
            pl.BlockSpec((1, STEP, order), lambda s, k: (s, k, 0)),
            pl.BlockSpec((1, STEP, modes), lambda s, k: (s, k, 0)),
        ],
        compiler_params=pltpu.CompilerParams(vmem_limit_bytes=52 << 20),
        out_specs=[VMEM] * 4
        + [pl.BlockSpec((1, modes, order), lambda s, k: (s, 0, 0))],
        out_shape=[held(count, HEAD)] * 4 + [jax.ShapeDtypeStruct((count, modes, order), F32)],
        scratch_shapes=[pltpu.VMEM((order, order), F32), pltpu.VMEM((STEP, order), jnp.bfloat16)],
        cost_estimate=pl.CostEstimate(
            flops=12 * count * 128 * 128 * inner * 2, bytes_accessed=14000000, transcendentals=0
        ),
        name="mass",
    )(mass_bb, im, cm, fm)


SMALL = pltpu.CompilerParams(vmem_limit_bytes=4 << 20)


def near(bufs):
    return [pltpu.with_memory_space_constraint(buf, pltpu.VMEM) for buf in bufs]


def held(count, rows):
    return pltpu.VMEM((count, rows, 128), F32)


def codes_of(slots):
    return [jnp.max(ref[n, HEAD : HEAD + 1, :]).astype(jnp.int32) for ref, n in slots]


def place():
    r = lax.axis_index("row")
    core = lax.rem(r, 2)
    x = lax.rem(r // 2, 4)
    y = r // 8
    u = jnp.where(core == 0, x, y)
    v = jnp.where(core == 0, y, x)
    return core, u, v


def pack_kernel(*refs):
    keys, ins, outs = refs[:4], refs[-8:-4], refs[-4:]
    core, u, v = place()
    if outs[0].shape[1] == PKT:
        empty = jnp.full((8, 128), -1.0, F32)
        for out in outs:
            for n in range(8):
                out[n, HEAD:PKT, :] = empty
    count = ins[0].shape[0]
    codes = codes_of([(ref, n) for ref in keys for n in range(count)])
    for n, code in enumerate(codes):
        owner = code // (BPO * 16)
        c = lax.rem(owner, 2)
        x = lax.rem(owner // 2, 4)
        y = owner // 8
        du = lax.rem(jnp.where(core == 0, x, y) - u + 4, 4)
        dv = lax.rem(jnp.where(core == 0, y, x) - v + 4, 4)
        slot = dv * 2 + lax.rem(c + core, 2)
        for k, out in enumerate(outs):

            @pl.when(du == k)
            def _(out=out, n=n, slot=slot):
                out[slot] = ins[n // count][n % count]


def pack(keys, bufs):
    bufs = keys if bufs is None else keys + bufs
    return pl.pallas_call(
        pack_kernel,
        in_specs=[VMEM] * len(bufs),
        out_specs=[VMEM] * 4,
        out_shape=[held(8, bufs[-1].shape[1])] * 4,
        compiler_params=SMALL,
        cost_estimate=pl.CostEstimate(flops=2000000, bytes_accessed=4000000, transcendentals=0),
        name="pack",
    )(*near(bufs))


def turn_kernel(*refs):
    ins, outs = refs[:4], refs[4:]
    for k in range(4):
        for q in range(1, 8):
            outs[q - 1][k] = ins[k][q]


def turn(bufs):
    return pl.pallas_call(
        turn_kernel,
        in_specs=[VMEM] * 4,
        out_specs=[VMEM] * 7,
        out_shape=[held(4, bufs[0].shape[1])] * 7,
        compiler_params=SMALL,
        cost_estimate=pl.CostEstimate(flops=2000000, bytes_accessed=6000000, transcendentals=0),
        name="turn",
    )(*near(bufs))


def sum_kernel(*refs):
    keys, ins, band = refs[:11], refs[-12:-1], refs[-1]

    def slots(some):
        return [(ref, 0) for ref in some[:4]] + [(ref, n) for ref in some[4:] for n in range(4)]

    codes = codes_of(slots(keys))
    band[...] = jnp.zeros_like(band)
    for (ref, n), code in zip(slots(ins), codes):

        @pl.when(code >= 0)
        def _(ref=ref, n=n, code=code):
            last = lax.rem(code, 4)
            mid = lax.rem(code // 4, 4)
            base = lax.rem(code // 16, BPO)
            marks = (0, mid, last)
            for p, (i, j) in enumerate(PAIRS):
                g = base + marks[i]
                d = marks[j] - marks[i]
                band[g, d] += ref[n, p * ROWS : (p + 1) * ROWS, :]


def assemble(keys, bufs):
    bufs = keys if bufs is None else keys + bufs
    return pl.pallas_call(
        sum_kernel,
        in_specs=[VMEM] * len(bufs),
        out_specs=VMEM,
        out_shape=jax.ShapeDtypeStruct((BPO, BAND, ROWS, 128), F32),
        compiler_params=SMALL,
        cost_estimate=pl.CostEstimate(flops=4000000, bytes_accessed=6000000, transcendentals=0),
        name="assemble",
    )(*near(bufs))


def spots():
    return [(r // 8, (r // 2) % 4, r % 2) for r in range(32)]


def row_of(y, x, c):
    return (y % 4) * 8 + (x % 4) * 2 + c


def first_turn(d):
    return [
        (r, row_of(y, x + d, c) if c == 0 else row_of(y + d, x, c))
        for r, (y, x, c) in enumerate(spots())
    ]


def second_turn(d, e):
    return [
        (r, row_of(y + d, x, c ^ e) if c == 0 else row_of(y, x + d, c ^ e))
        for r, (y, x, c) in enumerate(spots())
    ]


def over_col(bufs):
    return [bufs[0]] + [
        lax.ppermute(bufs[d], "col", [(z, (z + d) % 4) for z in range(4)]) for d in (1, 2, 3)
    ]


def over_u(keys, bufs):
    slots = pack(keys, bufs)
    two = lax.ppermute(slots[2], "row", first_turn(2))
    one = lax.ppermute(slots[1], "row", first_turn(1))
    three = lax.ppermute(slots[3], "row", first_turn(3))
    return [slots[0], one, two, three]


def over_v(slots):
    parts = turn(slots)
    return slots + [
        lax.ppermute(parts[q - 1], "row", second_turn(q // 2, q % 2))
        for q in (4, 2, 6, 5, 3, 7, 1)
    ]


def per_device(
    stiff_bb, stiff_bi, constraint_modes, interior_mass, fixed_modes, mass_bb, boundary_map
):
    k_out = k_packets(boundary_map, stiff_bb, stiff_bi, constraint_modes)
    k_in = over_col(k_out)
    *m_out, coupling = m_packets(mass_bb, interior_mass, constraint_modes, fixed_modes)
    m_in = over_col(m_out)
    k_half = over_u(k_in, None)
    m_half = over_u(k_in, m_in)
    k_end = over_v(k_half)
    m_end = over_v(m_half)
    band_k = assemble(k_end, None)
    band_m = assemble(k_end, m_end)
    return band_k, band_m, coupling


def solution(mesh):
    placed = (
        P(("row", "col"), None, None, None),
        P(("row", "col"), None, None),
        P(("row", "col"), None, None),
        P(("row", "col"), None),
        P(("row", "col"), None, None),
        P(("row", "col"), None, None, None),
        P(("row", "col"), None),
    )
    return jax.shard_map(
        per_device,
        mesh=mesh,
        in_specs=placed,
        out_specs=(
            P("row", None, "col", None),
            P("row", None, "col", None),
            P(("row", "col"), None, None),
        ),
        check_vma=False,
    )
```

```python
import functools

import jax
import jax.numpy as jnp
from jax import lax
from jax.experimental import pallas as pl
from jax.experimental.pallas import tpu as pltpu
from jax.sharding import PartitionSpec as P


BAND = 4
BPO = 24
PAIRS = ((0, 0), (1, 1), (2, 2), (0, 1), (0, 2), (1, 2))
ROWS = 32
HEAD = 6 * ROWS
PKT = HEAD + 8
STEP = 1024
SIDE = 8
HOP = 4


F32 = jnp.float32
VMEM = pl.BlockSpec(memory_space=pltpu.VMEM)
SMEM = pl.BlockSpec(memory_space=pltpu.SMEM)


def write_packets(s, total, map_ref, outs):
    me = lax.axis_index("col")
    for d, out in enumerate(outs):
        lane = lax.rem(me + d, 4)
        for p, (i, j) in enumerate(PAIRS):
            rows = pl.ds(pl.multiple_of(i * 128 + lane * ROWS, ROWS), ROWS)
            out[s, p * ROWS : (p + 1) * ROWS, :] = total[rows, j * 128 : (j + 1) * 128]
    if map_ref is not None:
        first = map_ref[s, 0]
        code = (first * 4 + map_ref[s, 1] - first) * 4 + map_ref[s, 2] - first
        head = jnp.full((8, 128), code.astype(F32), F32)
        for out in outs:
            out[s, HEAD:PKT, :] = head


def k_kernel(map_ref, bb, bi, cm, o0, o1, o2, o3, total):
    for i in range(3):
        total[i * 128 : (i + 1) * 128, :] = bb[0, i].astype(F32)
    total[0:128, :] += jnp.dot(bi[0, 0:128, :], cm[0], preferred_element_type=F32)
    total[128:384, 128:384] += jnp.dot(
        bi[0, 128:384, :], cm[0, :, 128:384], preferred_element_type=F32
    )
    write_packets(pl.program_id(0), total, map_ref, (o0, o1, o2, o3))


def k_packets(bmap, stiff_bb, stiff_bi, cm):
    count, order, inner = stiff_bi.shape
    return pl.pallas_call(
        k_kernel,
        grid=(count,),
        in_specs=[
            SMEM,
            pl.BlockSpec((1, 3, 128, order), lambda s: (s, 0, 0, 0)),
            pl.BlockSpec((1, order, inner), lambda s: (s, 0, 0)),
            pl.BlockSpec((1, inner, order), lambda s: (s, 0, 0)),
        ],
        out_specs=[VMEM] * 4,
        out_shape=[held(count, PKT)] * 4,
        scratch_shapes=[pltpu.VMEM((order, order), F32)],
        compiler_params=pltpu.CompilerParams(vmem_limit_bytes=56 << 20),
        cost_estimate=pl.CostEstimate(
            flops=6 * count * 128 * 128 * inner * 2, bytes_accessed=16000000, transcendentals=0
        ),
        name="stiffness",
    )(bmap, stiff_bb, stiff_bi, cm)


def m_kernel(steps, bb, im, cm, fm, o0, o1, o2, o3, coup, total, w):
    s, k = pl.program_id(0), pl.program_id(1)

    @pl.when(k == 0)
    def _():
        for i in range(3):
            total[i * 128 : (i + 1) * 128, :] = bb[0, i].astype(F32)
        coup[...] = jnp.zeros_like(coup)

    for j in range(STEP // 128):
        lines = im[:, pl.ds(pl.multiple_of(k * STEP + j * 128, 128), 128)]
        mine = lax.broadcasted_iota(jnp.int32, lines.shape, 0) == s
        line = jnp.sum(jnp.where(mine, lines, 0.0), axis=0, keepdims=True)
        column = jnp.broadcast_to(line, (128, 128)).T
        part = slice(j * 128, (j + 1) * 128)
        for i in range(3):
            lanes = slice(i * 128, (i + 1) * 128)
            w[part, lanes] = (column * cm[0, part, lanes].astype(F32)).astype(jnp.bfloat16)
    dims = (((0,), (0,)), ((), ()))
    total[0:128, :] += lax.dot_general(cm[0, :, 0:128], w[...], dims, preferred_element_type=F32)
    total[128:384, 128:384] += lax.dot_general(
        cm[0, :, 128:384], w[:, 128:384], dims, preferred_element_type=F32
    )
    coup[0] += lax.dot_general(fm[0], w[...], dims, preferred_element_type=F32)

    @pl.when(k == steps - 1)
    def _():
        write_packets(s, total, None, (o0, o1, o2, o3))


def m_packets(mass_bb, im, cm, fm):
    count, inner, order = cm.shape
    modes = fm.shape[2]
    steps = inner // STEP
    return pl.pallas_call(
        functools.partial(m_kernel, steps),
        grid=(count, steps),
        in_specs=[
            pl.BlockSpec((1, 3, 128, order), lambda s, k: (s, 0, 0, 0)),
            pl.BlockSpec((count, inner), lambda s, k: (0, 0)),
            pl.BlockSpec((1, STEP, order), lambda s, k: (s, k, 0)),
            pl.BlockSpec((1, STEP, modes), lambda s, k: (s, k, 0)),
        ],
        compiler_params=pltpu.CompilerParams(vmem_limit_bytes=52 << 20),
        out_specs=[VMEM] * 4
        + [pl.BlockSpec((1, modes, order), lambda s, k: (s, 0, 0))],
        out_shape=[held(count, HEAD)] * 4 + [jax.ShapeDtypeStruct((count, modes, order), F32)],
        scratch_shapes=[pltpu.VMEM((order, order), F32), pltpu.VMEM((STEP, order), jnp.bfloat16)],
        cost_estimate=pl.CostEstimate(
            flops=12 * count * 128 * 128 * inner * 2, bytes_accessed=14000000, transcendentals=0
        ),
        name="mass",
    )(mass_bb, im, cm, fm)


SMALL = pltpu.CompilerParams(vmem_limit_bytes=4 << 20)


def near(bufs):
    return [pltpu.with_memory_space_constraint(buf, pltpu.VMEM) for buf in bufs]


def held(count, rows):
    return pltpu.VMEM((count, rows, 128), F32)


def codes_of(slots):
    return [jnp.max(ref[n, HEAD : HEAD + 1, :]).astype(jnp.int32) for ref, n in slots]


def place():
    r = lax.axis_index("row")
    core = lax.rem(r, 2)
    x = lax.rem(r // 2, 4)
    y = r // 8
    u = jnp.where(core == 0, x, y)
    v = jnp.where(core == 0, y, x)
    return core, u, v


def way(code, spot):
    core, u, v = spot
    owner = code // (BPO * 16)
    c = lax.rem(owner, 2)
    x = lax.rem(owner // 2, 4)
    y = owner // 8
    du = lax.rem(jnp.where(core == 0, x, y) - u + 4, 4)
    dv = lax.rem(jnp.where(core == 0, y, x) - v + 4, 4)
    return du, dv * 2 + lax.rem(c + core, 2)


def slots_of(refs):
    return [(ref, n) for ref in refs for n in range(ref.shape[0])]


def clear(outs):
    if outs[0].shape[1] == PKT:
        for out, n in slots_of(outs):
            out[n, HEAD:PKT, :] = jnp.full((8, 128), -1.0, F32)


def pack_kernel(*refs):
    keys, ins, outs = refs[:4], refs[-6:-2], refs[-2:]
    spot = place()
    clear(outs)
    turns = [way(code, spot)[0] for code in codes_of(slots_of(keys))]
    ones = sum([(du == 1).astype(jnp.int32) for du in turns])
    twos = sum([(du == 2).astype(jnp.int32) for du in turns])
    ahead = jnp.minimum(jnp.minimum(HOP, twos), SIDE - ones)
    used = [jnp.int32(0), jnp.int32(0)]
    seen = jnp.int32(0)
    for (ref, n), du in zip(slots_of(ins), turns):
        far = du == 2
        early = far & (seen < ahead)
        seen = seen + far.astype(jnp.int32)
        for side, goes in enumerate(((du == 1) | early, (du == 3) | (far & ~early))):

            @pl.when(goes)
            def _(out=outs[side], ref=ref, n=n, slot=used[side]):
                out[slot] = ref[n]

            used[side] = used[side] + goes.astype(jnp.int32)


def hop_kernel(*refs):
    keys, ins, outs = refs[:2], refs[-4:-2], refs[-2:]
    spot = place()
    clear(outs)
    for key, src, out in zip(keys, ins, outs):
        used = jnp.int32(0)
        for (ref, n), code in zip(slots_of([src]), codes_of(slots_of([key]))):
            goes = (code >= 0) & (way(code, spot)[0] != 0)

            @pl.when(goes)
            def _(out=out, ref=ref, n=n, slot=used):
                out[slot] = ref[n]

            used = used + goes.astype(jnp.int32)


def turn_kernel(*refs):
    keys, ins, outs, used = refs[:8], refs[-17:-9], refs[-9:-1], refs[-1]
    spot = place()
    clear(outs)
    for q in range(8):
        used[q] = 0
    for (ref, n), code in zip(slots_of(ins), codes_of(slots_of(keys))):
        du, where = way(code, spot)

        @pl.when((code >= 0) & (du == 0))
        def _(ref=ref, n=n, where=where):
            slot = used[where]
            used[where] = slot + 1
            for q in range(8):

                @pl.when(where == q)
                def _(out=outs[q]):
                    out[slot] = ref[n]


def route(kernel, keys, bufs, sizes, scratch=()):
    ins = list(keys) if bufs is None else list(keys) + list(bufs)
    return pl.pallas_call(
        kernel,
        in_specs=[VMEM] * len(ins),
        out_specs=[VMEM] * len(sizes),
        out_shape=[held(n, ins[-1].shape[1]) for n in sizes],
        scratch_shapes=list(scratch),
        compiler_params=SMALL,
        cost_estimate=pl.CostEstimate(flops=2000000, bytes_accessed=4000000, transcendentals=0),
    )(*near(ins))


def sum_kernel(*refs):
    keys, ins, band = refs[:8], refs[-9:-1], refs[-1]
    codes = codes_of(slots_of(keys))
    band[...] = jnp.zeros_like(band)
    for (ref, n), code in zip(slots_of(ins), codes):

        @pl.when(code >= 0)
        def _(ref=ref, n=n, code=code):
            last = lax.rem(code, 4)
            mid = lax.rem(code // 4, 4)
            base = lax.rem(code // 16, BPO)
            marks = (0, mid, last)
            for p, (i, j) in enumerate(PAIRS):
                g = base + marks[i]
                d = marks[j] - marks[i]
                band[g, d] += ref[n, p * ROWS : (p + 1) * ROWS, :]


def assemble(keys, bufs):
    bufs = keys if bufs is None else keys + bufs
    return pl.pallas_call(
        sum_kernel,
        in_specs=[VMEM] * len(bufs),
        out_specs=VMEM,
        out_shape=jax.ShapeDtypeStruct((BPO, BAND, ROWS, 128), F32),
        compiler_params=SMALL,
        cost_estimate=pl.CostEstimate(flops=4000000, bytes_accessed=6000000, transcendentals=0),
        name="assemble",
    )(*near(bufs))


def spots():
    return [(r // 8, (r // 2) % 4, r % 2) for r in range(32)]


def row_of(y, x, c):
    return (y % 4) * 8 + (x % 4) * 2 + c


def first_turn(d):
    return [
        (r, row_of(y, x + d, c) if c == 0 else row_of(y + d, x, c))
        for r, (y, x, c) in enumerate(spots())
    ]


def second_turn(d, e):
    return [
        (r, row_of(y + d, x, c ^ e) if c == 0 else row_of(y, x + d, c ^ e))
        for r, (y, x, c) in enumerate(spots())
    ]


def over_col(bufs):
    return [bufs[0]] + [
        lax.ppermute(bufs[d], "col", [(z, (z + d) % 4) for z in range(4)]) for d in (2, 1, 3)
    ]


def beside(bufs, axis):
    return [lax.ppermute(bufs[0], axis, first_turn(1)), lax.ppermute(bufs[1], axis, first_turn(3))]


def over_v(parts):
    return [parts[0]] + [
        lax.ppermute(parts[q], "row", second_turn(q // 2, q % 2)) for q in (4, 2, 6, 5, 3, 7, 1)
    ]


def per_device(
    stiff_bb, stiff_bi, constraint_modes, interior_mass, fixed_modes, mass_bb, boundary_map
):
    k_out = k_packets(boundary_map, stiff_bb, stiff_bi, constraint_modes)
    k_in = over_col(k_out)
    *m_out, coupling = m_packets(mass_bb, interior_mass, constraint_modes, fixed_modes)
    m_in = over_col(m_out)
    flow = {"k": {"in": k_in}, "m": {"in": m_in}}

    def stage(kernel, name, took, sizes, scratch=()):
        for tag in ("k", "m"):
            keys = [b for t in took for b in flow["k"][t]]
            bufs = None if tag == "k" else [b for t in took for b in flow[tag][t]]
            flow[tag][name] = route(kernel, keys, bufs, sizes, scratch)

    def move(name, made, send):
        for tag in ("k", "m"):
            flow[tag][name] = send(flow[tag][made])

    stage(pack_kernel, "pack", ("in",), (SIDE, SIDE))
    move("near", "pack", lambda bufs: beside(bufs, "row"))
    stage(hop_kernel, "hop", ("near",), (HOP, HOP))
    move("next", "hop", lambda bufs: beside(bufs, "row"))
    stage(turn_kernel, "turn", ("in", "near", "next"), (4,) * 8, (pltpu.SMEM((8,), jnp.int32),))
    move("last", "turn", over_v)
    band_k = assemble(flow["k"]["last"], None)
    band_m = assemble(flow["k"]["last"], flow["m"]["last"])
    return band_k, band_m, coupling


def solution(mesh):
    placed = (
        P(("row", "col"), None, None, None),
        P(("row", "col"), None, None),
        P(("row", "col"), None, None),
        P(("row", "col"), None),
        P(("row", "col"), None, None),
        P(("row", "col"), None, None, None),
        P(("row", "col"), None),
    )
    return jax.shard_map(
        per_device,
        mesh=mesh,
        in_specs=placed,
        out_specs=(
            P("row", None, "col", None),
            P("row", None, "col", None),
            P(("row", "col"), None, None),
        ),
        check_vma=False,
    )
```

```python
import jax
import jax.numpy as jnp
from jax import lax
from jax.experimental import pallas as pl
from jax.experimental.pallas import tpu as pltpu
from jax.sharding import PartitionSpec as P


BAND = 4
BPO = 24
PAIRS = ((0, 0), (1, 1), (2, 2), (0, 1), (0, 2), (1, 2))
ROWS = 32
HEAD = 6 * ROWS
PKT = HEAD + 8
SIDE = 8
HOP = 4


F32 = jnp.float32
VMEM = pl.BlockSpec(memory_space=pltpu.VMEM)
SMEM = pl.BlockSpec(memory_space=pltpu.SMEM)


def write_packets(s, total, map_ref, outs):
    me = lax.axis_index("col")
    for d, out in enumerate(outs):
        lane = lax.rem(me + d, 4)
        for p, (i, j) in enumerate(PAIRS):
            rows = pl.ds(pl.multiple_of(i * 128 + lane * ROWS, ROWS), ROWS)
            out[s, p * ROWS : (p + 1) * ROWS, :] = total[rows, j * 128 : (j + 1) * 128]
    if map_ref is not None:
        first = map_ref[s, 0]
        code = (first * 4 + map_ref[s, 1] - first) * 4 + map_ref[s, 2] - first
        head = jnp.full((8, 128), code.astype(F32), F32)
        for out in outs:
            out[s, HEAD:PKT, :] = head


def k_kernel(map_ref, bb, bi, cm, o0, o1, o2, o3, total):
    for i in range(3):
        total[i * 128 : (i + 1) * 128, :] = bb[0, i].astype(F32)
    total[0:128, :] += jnp.dot(bi[0, 0:128, :], cm[0], preferred_element_type=F32)
    total[128:384, 128:384] += jnp.dot(
        bi[0, 128:384, :], cm[0, :, 128:384], preferred_element_type=F32
    )
    write_packets(pl.program_id(0), total, map_ref, (o0, o1, o2, o3))


def k_packets(bmap, stiff_bb, stiff_bi, cm):
    count, order, inner = stiff_bi.shape
    return pl.pallas_call(
        k_kernel,
        grid=(count,),
        in_specs=[
            SMEM,
            pl.BlockSpec((1, 3, 128, order), lambda s: (s, 0, 0, 0)),
            pl.BlockSpec((1, order, inner), lambda s: (s, 0, 0)),
            pl.BlockSpec((1, inner, order), lambda s: (s, 0, 0)),
        ],
        out_specs=[VMEM] * 4,
        out_shape=[held(count, PKT)] * 4,
        scratch_shapes=[pltpu.VMEM((order, order), F32)],
        compiler_params=pltpu.CompilerParams(vmem_limit_bytes=56 << 20),
        cost_estimate=pl.CostEstimate(
            flops=6 * count * 128 * 128 * inner * 2, bytes_accessed=16000000, transcendentals=0
        ),
        name="stiffness",
    )(bmap, stiff_bb, stiff_bi, cm)


def weigh(s, im, cm, w):
    for j in range(w.shape[0] // 128):
        part = slice(j * 128, (j + 1) * 128)
        lines = im[:, part]
        mine = lax.broadcasted_iota(jnp.int32, lines.shape, 0) == s
        line = jnp.sum(jnp.where(mine, lines, 0.0), axis=0, keepdims=True)
        column = jnp.broadcast_to(line, (128, 128)).T
        for i in range(w.shape[1] // 128):
            lanes = slice(i * 128, (i + 1) * 128)
            w[part, lanes] = (column * cm[0, part, lanes].astype(F32)).astype(jnp.bfloat16)


DOWN = (((0,), (0,)), ((), ()))


def m_kernel(bb, im, cm, o0, o1, o2, o3, total, w):
    s = pl.program_id(0)
    weigh(s, im, cm, w)
    for i in range(3):
        total[i * 128 : (i + 1) * 128, :] = bb[0, i].astype(F32)
    total[0:128, :] += lax.dot_general(cm[0, :, 0:128], w[...], DOWN, preferred_element_type=F32)
    total[128:384, 128:384] += lax.dot_general(
        cm[0, :, 128:384], w[:, 128:384], DOWN, preferred_element_type=F32
    )
    write_packets(s, total, None, (o0, o1, o2, o3))


def m_packets(mass_bb, im, cm):
    count, inner, order = cm.shape
    return pl.pallas_call(
        m_kernel,
        grid=(count,),
        in_specs=[
            pl.BlockSpec((1, 3, 128, order), lambda s: (s, 0, 0, 0)),
            pl.BlockSpec((count, inner), lambda s: (0, 0)),
            pl.BlockSpec((1, inner, order), lambda s: (s, 0, 0)),
        ],
        out_specs=[VMEM] * 4,
        out_shape=[held(count, HEAD)] * 4,
        compiler_params=pltpu.CompilerParams(vmem_limit_bytes=52 << 20),
        scratch_shapes=[pltpu.VMEM((order, order), F32), pltpu.VMEM((inner, order), jnp.bfloat16)],
        cost_estimate=pl.CostEstimate(
            flops=6 * count * 128 * 128 * inner * 2, bytes_accessed=9000000, transcendentals=0
        ),
        name="mass",
    )(mass_bb, im, cm)


def c_kernel(im, cm, fm, coup, w):
    weigh(pl.program_id(0), im, cm, w)
    coup[0] = lax.dot_general(fm[0], w[...], DOWN, preferred_element_type=F32)


def couple(im, cm, fm):
    count, inner, order = cm.shape
    modes = fm.shape[2]
    return pl.pallas_call(
        c_kernel,
        grid=(count,),
        in_specs=[
            pl.BlockSpec((count, inner), lambda s: (0, 0)),
            pl.BlockSpec((1, inner, order), lambda s: (s, 0, 0)),
            pl.BlockSpec((1, inner, modes), lambda s: (s, 0, 0)),
        ],
        out_specs=pl.BlockSpec((1, modes, order), lambda s: (s, 0, 0)),
        out_shape=jax.ShapeDtypeStruct((count, modes, order), F32),
        compiler_params=pltpu.CompilerParams(vmem_limit_bytes=40 << 20),
        scratch_shapes=[pltpu.VMEM((inner, order), jnp.bfloat16)],
        cost_estimate=pl.CostEstimate(
            flops=6 * count * 128 * 128 * inner * 2, bytes_accessed=12000000, transcendentals=0
        ),
        name="couple",
    )(im, cm, fm)


SMALL = pltpu.CompilerParams(vmem_limit_bytes=4 << 20)


def near(bufs):
    return [pltpu.with_memory_space_constraint(buf, pltpu.VMEM) for buf in bufs]


def held(count, rows):
    return pltpu.VMEM((count, rows, 128), F32)


def codes_of(slots):
    return [jnp.max(ref[n, HEAD : HEAD + 1, :]).astype(jnp.int32) for ref, n in slots]


def place():
    r = lax.axis_index("row")
    core = lax.rem(r, 2)
    x = lax.rem(r // 2, 4)
    y = r // 8
    u = jnp.where(core == 0, x, y)
    v = jnp.where(core == 0, y, x)
    return core, u, v


def way(code, spot):
    core, u, v = spot
    owner = code // (BPO * 16)
    c = lax.rem(owner, 2)
    x = lax.rem(owner // 2, 4)
    y = owner // 8
    du = lax.rem(jnp.where(core == 0, x, y) - u + 4, 4)
    dv = lax.rem(jnp.where(core == 0, y, x) - v + 4, 4)
    return du, dv * 2 + lax.rem(c + core, 2)


def slots_of(refs):
    return [(ref, n) for ref in refs for n in range(ref.shape[0])]


def clear(outs):
    if outs[0].shape[1] == PKT:
        for out, n in slots_of(outs):
            out[n, HEAD:PKT, :] = jnp.full((8, 128), -1.0, F32)


def pack_kernel(*refs):
    keys, ins, outs = refs[:4], refs[-6:-2], refs[-2:]
    spot = place()
    clear(outs)
    turns = [way(code, spot)[0] for code in codes_of(slots_of(keys))]
    ones = sum([(du == 1).astype(jnp.int32) for du in turns])
    twos = sum([(du == 2).astype(jnp.int32) for du in turns])
    ahead = jnp.minimum(jnp.minimum(HOP, twos), SIDE - ones)
    used = [jnp.int32(0), jnp.int32(0)]
    seen = jnp.int32(0)
    for (ref, n), du in zip(slots_of(ins), turns):
        far = du == 2
        early = far & (seen < ahead)
        seen = seen + far.astype(jnp.int32)
        for side, goes in enumerate(((du == 1) | early, (du == 3) | (far & ~early))):

            @pl.when(goes)
            def _(out=outs[side], ref=ref, n=n, slot=used[side]):
                out[slot] = ref[n]

            used[side] = used[side] + goes.astype(jnp.int32)


def hop_kernel(*refs):
    keys, ins, outs = refs[:2], refs[-4:-2], refs[-2:]
    spot = place()
    clear(outs)
    for key, src, out in zip(keys, ins, outs):
        used = jnp.int32(0)
        for (ref, n), code in zip(slots_of([src]), codes_of(slots_of([key]))):
            goes = (code >= 0) & (way(code, spot)[0] != 0)

            @pl.when(goes)
            def _(out=out, ref=ref, n=n, slot=used):
                out[slot] = ref[n]

            used = used + goes.astype(jnp.int32)


def turn_kernel(*refs):
    keys, ins, outs, used = refs[:8], refs[-17:-9], refs[-9:-1], refs[-1]
    spot = place()
    clear(outs)
    for q in range(8):
        used[q] = 0
    for (ref, n), code in zip(slots_of(ins), codes_of(slots_of(keys))):
        du, where = way(code, spot)

        @pl.when((code >= 0) & (du == 0))
        def _(ref=ref, n=n, where=where):
            slot = used[where]
            used[where] = slot + 1
            for q in range(8):

                @pl.when(where == q)
                def _(out=outs[q]):
                    out[slot] = ref[n]


def route(kernel, keys, bufs, sizes, scratch=()):
    ins = list(keys) if bufs is None else list(keys) + list(bufs)
    return pl.pallas_call(
        kernel,
        in_specs=[VMEM] * len(ins),
        out_specs=[VMEM] * len(sizes),
        out_shape=[held(n, ins[-1].shape[1]) for n in sizes],
        scratch_shapes=list(scratch),
        compiler_params=SMALL,
        cost_estimate=pl.CostEstimate(flops=2000000, bytes_accessed=4000000, transcendentals=0),
    )(*near(ins))


def sum_kernel(*refs):
    keys, ins, band = refs[:8], refs[-9:-1], refs[-1]
    codes = codes_of(slots_of(keys))
    band[...] = jnp.zeros_like(band)
    for (ref, n), code in zip(slots_of(ins), codes):

        @pl.when(code >= 0)
        def _(ref=ref, n=n, code=code):
            last = lax.rem(code, 4)
            mid = lax.rem(code // 4, 4)
            base = lax.rem(code // 16, BPO)
            marks = (0, mid, last)
            for p, (i, j) in enumerate(PAIRS):
                g = base + marks[i]
                d = marks[j] - marks[i]
                band[g, d] += ref[n, p * ROWS : (p + 1) * ROWS, :]


def assemble(keys, bufs):
    bufs = keys if bufs is None else keys + bufs
    return pl.pallas_call(
        sum_kernel,
        in_specs=[VMEM] * len(bufs),
        out_specs=VMEM,
        out_shape=jax.ShapeDtypeStruct((BPO, BAND, ROWS, 128), F32),
        compiler_params=SMALL,
        cost_estimate=pl.CostEstimate(flops=4000000, bytes_accessed=6000000, transcendentals=0),
        name="assemble",
    )(*near(bufs))


def spots():
    return [(r // 8, (r // 2) % 4, r % 2) for r in range(32)]


def row_of(y, x, c):
    return (y % 4) * 8 + (x % 4) * 2 + c


def first_turn(d):
    return [
        (r, row_of(y, x + d, c) if c == 0 else row_of(y + d, x, c))
        for r, (y, x, c) in enumerate(spots())
    ]


def second_turn(d, e):
    return [
        (r, row_of(y + d, x, c ^ e) if c == 0 else row_of(y, x + d, c ^ e))
        for r, (y, x, c) in enumerate(spots())
    ]


def over_col(bufs):
    return [bufs[0]] + [
        lax.ppermute(bufs[d], "col", [(z, (z + d) % 4) for z in range(4)]) for d in (2, 1, 3)
    ]


def beside(bufs, axis):
    return [lax.ppermute(bufs[0], axis, first_turn(1)), lax.ppermute(bufs[1], axis, first_turn(3))]


def over_v(parts):
    return [parts[0]] + [
        lax.ppermute(parts[q], "row", second_turn(q // 2, q % 2)) for q in (4, 2, 6, 5, 3, 7, 1)
    ]


def per_device(
    stiff_bb, stiff_bi, constraint_modes, interior_mass, fixed_modes, mass_bb, boundary_map
):
    k_out = k_packets(boundary_map, stiff_bb, stiff_bi, constraint_modes)
    k_in = over_col(k_out)
    m_out = m_packets(mass_bb, interior_mass, constraint_modes)
    m_in = over_col(m_out)
    flow = {"k": {"in": k_in}, "m": {"in": m_in}}

    def stage(kernel, name, took, sizes, scratch=()):
        for tag in ("k", "m"):
            keys = [b for t in took for b in flow["k"][t]]
            bufs = None if tag == "k" else [b for t in took for b in flow[tag][t]]
            flow[tag][name] = route(kernel, keys, bufs, sizes, scratch)

    def move(name, made, send):
        for tag in ("k", "m"):
            flow[tag][name] = send(flow[tag][made])

    stage(pack_kernel, "pack", ("in",), (SIDE, SIDE))
    move("near", "pack", lambda bufs: beside(bufs, "row"))
    stage(hop_kernel, "hop", ("near",), (HOP, HOP))
    move("next", "hop", lambda bufs: beside(bufs, "row"))
    stage(turn_kernel, "turn", ("in", "near", "next"), (4,) * 8, (pltpu.SMEM((8,), jnp.int32),))
    move("last", "turn", over_v)
    coupling = couple(interior_mass, constraint_modes, fixed_modes)
    band_k = assemble(flow["k"]["last"], None)
    band_m = assemble(flow["k"]["last"], flow["m"]["last"])
    return band_k, band_m, coupling


def solution(mesh):
    placed = (
        P(("row", "col"), None, None, None),
        P(("row", "col"), None, None),
        P(("row", "col"), None, None),
        P(("row", "col"), None),
        P(("row", "col"), None, None),
        P(("row", "col"), None, None, None),
        P(("row", "col"), None),
    )
    return jax.shard_map(
        per_device,
        mesh=mesh,
        in_specs=placed,
        out_specs=(
            P("row", None, "col", None),
            P("row", None, "col", None),
            P(("row", "col"), None, None),
        ),
        check_vma=False,
    )
```
